32 devices in a mesh: row: 8 (over z, y), col: 4 (over x, core).
Axes of the slice: x: 2, y: 2, z: 4, core: 2. Of those that a mesh axis runs over, the one named last changes fastest.
Arguments:
- interior_factor: float32 [8, 4, 1, 384, 384], P('row', 'col'), as said below
- coupling_in: bfloat16 [8, 4, 1, 384, 2048], P('row', 'col'), may hold values from -1.5 to 1.5
- coupling_back: bfloat16 [8, 4, 1, 384, 2048], P('row', 'col'), may hold values from -1.5 to 1.5
- interface_block: bfloat16 [8, 4, 1, 2048, 2048], P('row', 'col'), may hold values from -6 to 6
- gran_count: int32 [8, 4, 1], replicated, may hold values from 2 to 16, as said below
- gran_index: int32 [8, 4, 1, 16], replicated, may hold values from 0 to 15, as said below
Outputs:
- schur: float32 [8, 3, 1024, 1024], P('row', None, 'col')
The draws below stay inside these ranges and needn't reach their ends.
Inputs may be any that keep to these rules, and one draw needn't show every extreme that they name: `gran_count`: each entry is an even number of granules; in every row group some subdomain has 16. `gran_index`: each row is an order of the 16 window granules, each once; window granule p of row group r is global granule 8 * r + p modulo 8 * 8; the first gran_count entries are the subdomain's interface granules. `interior_factor`: lower triangular with a positive diagonal.
All inputs are finite; a program needn't handle non-finite values.
Results may differ from the reference program's by a relative error of at most 0.0003.
Values may be sent and summed in bfloat16 or wider, within the bound.
A program may use at most 128 MiB of HBM per device.

```python
import math
import jax
import jax.numpy as jnp
from jax import lax

NI = 384
SUB_DEV = 1
WING = 16
GMAX = 2048
N_ROW = 8
N_COL = 4


def draw_interior_factor(key, part):
    first, second = jax.random.split(key)
    shape = (N_ROW, N_COL, SUB_DEV, NI, NI)
    diagonal = jax.random.uniform(first, shape[:-1], jnp.float32, 1.5, 3.0)
    spread = jax.random.normal(second, shape, jnp.float32) * (0.5 / math.sqrt(NI))
    return jnp.tril(spread, -1) + diagonal[..., None] * jnp.eye(NI, dtype=jnp.float32)


def draw_gran_count(key, part):
    first, second, third = jax.random.split(jax.random.fold_in(key, 11), 3)
    shape = (N_ROW, N_COL, SUB_DEV)
    factor_one = jax.random.randint(first, shape, 0, 4)
    factor_two = jax.random.randint(second, shape, 0, 4)
    blocks = 1 + factor_one * factor_two // 3
    chosen = jax.random.randint(third, (N_ROW,), 0, N_COL)
    columns = jnp.arange(N_COL, dtype=jnp.int32)
    subs = jnp.arange(SUB_DEV, dtype=jnp.int32)
    forced = (columns[None, :, None] == chosen[:, None, None]) & (subs[None, None, :] == 0)
    blocks = jnp.where(forced, WING // 2, blocks)
    return (2 * blocks).astype(jnp.int32)


def draw_gran_index(key, part):
    scores = jax.random.randint(jax.random.fold_in(key, 23), (N_ROW, N_COL, SUB_DEV, WING), 0, 1 << 20)
    scored = scores * WING + jnp.arange(WING, dtype=jnp.int32)
    return jnp.argsort(scored, axis=-1, stable=True).astype(jnp.int32)


def level_of(key, shape, cuts, low, largest):
    factor_of = 1.0
    for axis_at, parts in cuts:
        draws = jax.random.uniform(jax.random.fold_in(jax.random.fold_in(key, 6), axis_at), (parts,), jnp.float32, low / len(cuts), largest / len(cuts))
        factor_of = factor_of * jnp.repeat(jnp.exp(draws), shape[axis_at] // parts).reshape((-1,) + (1,) * (len(shape) - 1 - axis_at))
    return factor_of


def scatter_about(key, dims, scale, reach, cuts=(), held_as=jnp.bfloat16):
    values = scale * jax.random.normal(key, dims, jnp.float32)
    if cuts:
        values = values * level_of(key, dims, cuts, -0.22, 0.18)
    return jnp.clip(values, -reach, reach).astype(held_as)


def setup_inputs(seed: int = 0) -> dict:
    streams_of = jax.random.split(jax.random.key(seed), 7)
    interior_factor = draw_interior_factor(jax.random.fold_in(streams_of[6], 71), 0)
    coupling_in = scatter_about(streams_of[1], (N_ROW, N_COL, SUB_DEV, NI, GMAX), 0.25, 1.5, ((0, 8), (1, 4)))
    coupling_back = scatter_about(streams_of[2], (N_ROW, N_COL, SUB_DEV, NI, GMAX), 0.25, 1.5, ((0, 8), (1, 4)))
    interface_block = scatter_about(streams_of[3], (N_ROW, N_COL, SUB_DEV, GMAX, GMAX), 1.0, 6.0, ((0, 8), (1, 4)))
    gran_count = draw_gran_count(jax.random.fold_in(streams_of[6], 71), 0)
    gran_index = draw_gran_index(jax.random.fold_in(streams_of[6], 71), 0)
    return dict(interior_factor=interior_factor, coupling_in=coupling_in, coupling_back=coupling_back, interface_block=interface_block, gran_count=gran_count, gran_index=gran_index)


def select_table(count, index):
    slots = jnp.arange(index.shape[0], dtype=jnp.int32)
    live = (slots < count).astype(jnp.float32)
    return (index[:, None] == slots[None, :]).astype(jnp.float32) * live[:, None]

def place(local, table):
    wing = table.shape[0]
    width = local.shape[0]
    granule = width // wing
    blocks = local.reshape(wing, granule, wing, granule)
    moved = jnp.einsum('ap,aibj,bq->piqj', table, blocks, table, precision=lax.Precision.HIGHEST)
    return moved.reshape(width, width)

def contribution(factor, coupling_in, coupling_back, interface_block, count, index):
    solved_in = lax.linalg.triangular_solve(factor, coupling_in.astype(jnp.float32), left_side=True, lower=True).astype(jnp.bfloat16)
    solved_back = lax.linalg.triangular_solve(factor, coupling_back.astype(jnp.float32), left_side=True, lower=True).astype(jnp.bfloat16)
    product = jnp.dot(solved_back.astype(jnp.float32).T, solved_in.astype(jnp.float32), precision=lax.Precision.HIGHEST)
    local = interface_block.astype(jnp.float32) - product
    return place(local, select_table(count, index))

def reference(interior_factor, coupling_in, coupling_back, interface_block, gran_count, gran_index):
    width = coupling_in.shape[-1]
    half = width // 2

    def group_window(pieces):
        factor, inner, back, own_block, counts, index = pieces
        factor = factor.reshape((-1,) + factor.shape[-2:])
        inner = inner.reshape((-1,) + inner.shape[-2:])
        back = back.reshape((-1,) + back.shape[-2:])
        own_block = own_block.reshape((-1,) + own_block.shape[-2:])
        counts = counts.reshape(-1)
        index = index.reshape((-1, index.shape[-1]))

        def accumulate(total, item):
            return (total + contribution(*item), None)
        total, unused = lax.scan(accumulate, jnp.zeros((width, width), jnp.float32), (factor, inner, back, own_block, counts, index))
        return total
    windows = lax.map(group_window, (interior_factor, coupling_in, coupling_back, interface_block, gran_count, gran_index))
    earlier = jnp.roll(windows, 1, axis=0)
    diagonal = windows[:, :half, :half] + earlier[:, half:, half:]
    return jnp.stack([diagonal, windows[:, :half, half:], windows[:, half:, :half]], axis=1)
```

```python
import functools

import jax
import jax.numpy as jnp
from jax import lax
from jax.experimental import pallas as pl
from jax.experimental.pallas import tpu as pltpu
from jax.sharding import PartitionSpec as P

MESH = pl.DeviceIdType.MESH
HIGHEST = lax.Precision.HIGHEST


def exact_dot(a, b):
    return jnp.dot(a, b, precision=HIGHEST, preferred_element_type=jnp.float32)


def invert_tile(tile):
    size = tile.shape[0]
    i = lax.broadcasted_iota(jnp.int32, tile.shape, 0)
    j = lax.broadcasted_iota(jnp.int32, tile.shape, 1)
    inverse = jnp.where(i == j, 1.0 / jnp.where(i == j, tile, 1.0), 0.0)
    k = 1
    while k < size:
        both = 2 * k
        mask = (i // both == j // both) & (i % both >= k) & (j % both < k)
        below = jnp.where(mask, tile, 0.0)
        inverse = inverse - exact_dot(inverse, exact_dot(below, inverse))
        k = both
    return inverse


def invert_lower(factor_ref, tile, inverse_refs):
    count = factor_ref.shape[0] // tile
    at = lambda b: pl.ds(b * tile, tile)
    diagonal = [invert_tile(factor_ref[at(b), at(b)]) for b in range(count)]
    tiles = {}
    for col in range(count):
        tiles[col, col] = diagonal[col]
        for row in range(col + 1, count):
            total = exact_dot(factor_ref[at(row), at(col)], tiles[col, col])
            for mid in range(col + 1, row):
                total = total + exact_dot(factor_ref[at(row), at(mid)], tiles[mid, col])
            tiles[row, col] = -exact_dot(diagonal[row], total)
    for row in range(count):
        for col in range(count):
            rest = tiles[row, col] if col <= row else jnp.zeros((tile, tile), jnp.float32)
            for ref in inverse_refs:
                piece = rest.astype(jnp.bfloat16)
                ref[at(row), at(col)] = piece
                rest = rest - piece.astype(jnp.float32)


def assemble_kernel(
    granule, tile, slot_ref, live_ref, factor_ref, in_ref, back_ref, own_ref, out_ref,
    high_ref, mid_ref, low_ref, placed_in, placed_back,
):
    wing = placed_in.shape[1] // granule
    p = pl.program_id(0)

    def granule_of(ref, q):
        return ref[:, pl.ds(pl.multiple_of(slot_ref[q] * granule, granule), granule)]

    @pl.when(p == 0)
    def _():
        invert_lower(factor_ref, tile, (high_ref, mid_ref, low_ref))
        step = 4 if wing % 4 == 0 else 1
        for source, target in ((in_ref, placed_in), (back_ref, placed_back)):
            for first in range(0, wing, step):
                pieces = []
                for q in range(first, first + step):
                    piece = granule_of(source, q)
                    pieces.append(jnp.where(live_ref[q] == 1, piece, jnp.zeros_like(piece)))
                coupling = jnp.concatenate(pieces, axis=1) if step > 1 else pieces[0]
                solved = sum(
                    jnp.dot(ref[...], coupling, preferred_element_type=jnp.float32)
                    for ref in (low_ref, mid_ref, high_ref)
                )
                target[:, pl.ds(first * granule, step * granule)] = solved.astype(jnp.bfloat16)

    @pl.when(live_ref[p] == 1)
    def _():
        columns = placed_back[:, pl.ds(pl.multiple_of(p * granule, granule), granule)]
        product = lax.dot_general(
            columns, placed_in[...], (((0,), (0,)), ((), ())), preferred_element_type=jnp.float32
        )
        for q in range(wing):
            block = granule_of(own_ref, q).astype(jnp.float32)
            block = jnp.where(live_ref[q] == 1, block, 0.0)
            out_ref[:, q * granule:(q + 1) * granule] = (
                block - product[:, q * granule:(q + 1) * granule]
            )

    @pl.when(live_ref[p] != 1)
    def _():
        out_ref[...] = jnp.zeros_like(out_ref)


def assemble(slot, live, factor, inner, back, own):
    ni, width = inner.shape
    wing = slot.shape[0]
    granule = width // wing
    tile = 128 if ni % 128 == 0 else ni
    whole = lambda shape: pl.BlockSpec(shape, lambda p, s, l: (0, 0))
    return pl.pallas_call(
        functools.partial(assemble_kernel, granule, tile),
        grid_spec=pltpu.PrefetchScalarGridSpec(
            num_scalar_prefetch=2,
            grid=(wing,),
            in_specs=[
                whole((ni, ni)),
                whole((ni, width)),
                whole((ni, width)),
                pl.BlockSpec((granule, width), lambda p, s, l: (s[p], 0)),
            ],
            out_specs=pl.BlockSpec((granule, width), lambda p, s, l: (p, 0)),
            scratch_shapes=[pltpu.VMEM((ni, ni), jnp.bfloat16)] * 3
            + [pltpu.VMEM((ni, width), jnp.bfloat16)] * 2,
        ),
        out_shape=jax.ShapeDtypeStruct((width, width), jnp.float32),
        compiler_params=pltpu.CompilerParams(vmem_limit_bytes=40 * 2**20),
    )(slot, live, factor, inner, back, own)


def exchange_kernel(
    n_row, n_col, w_ref, out_ref,
    mine, paired, arrived, carried,
    load_sem, send1, recv1, send2, recv2, send3, recv3,
):
    chips = n_col // 2
    rows, half = mine.shape[2], mine.shape[3]
    r = lax.axis_index("row")
    c = lax.axis_index("col")
    chip, core = c // 2, c % 2
    partner = chip * 2 + (1 - core)
    after = lax.rem(r + 1, n_row)
    before = lax.rem(r + n_row - 1, n_row)

    barrier = pltpu.get_barrier_semaphore()
    greet = [(r, partner), (after, c), (before, c)]
    greet += [(r, lax.rem(chip + o, chips) * 2 + core) for o in range(1, chips)]
    for device in greet:
        pl.semaphore_signal(barrier, inc=1, device_id=device, device_id_type=MESH)

    order = [3, 2, 1, 0]
    offsets = list(range(1, chips)) + [0]

    def part(q, o, which):
        device = lax.rem(chip + o, chips) * 2 + which
        return w_ref.at[q // 2, device, :, pl.ds((q % 2) * half, half)]

    loads, first, second = {}, {}, {}
    for q in order:
        for o in offsets:
            loads[q, o] = pltpu.make_async_copy(part(q, o, core), mine.at[q, o], load_sem.at[q, o])
            loads[q, o].start()
    pl.semaphore_wait(barrier, len(greet))
    for q in order:
        for o in offsets:
            first[q, o] = pltpu.make_async_remote_copy(
                src_ref=part(q, o, 1 - core), dst_ref=paired.at[q, o],
                send_sem=send1.at[q, o], recv_sem=recv1.at[q, o],
                device_id=(r, partner), device_id_type=MESH,
            )
            first[q, o].start()
    for q in order:
        for o in offsets:
            loads[q, o].wait()
            first[q, o].wait_recv()
            mine[q, o] = mine[q, o] + paired[q, o]
            if o:
                device = lax.rem(chip + o, chips) * 2 + core
                second[q, o] = pltpu.make_async_remote_copy(
                    src_ref=mine.at[q, o], dst_ref=arrived.at[q, o - 1],
                    send_sem=send2.at[q, o - 1], recv_sem=recv2.at[q, o - 1],
                    device_id=(r, device), device_id_type=MESH,
                )
                second[q, o].start()
    carry = pltpu.make_async_remote_copy(
        src_ref=mine.at[3, 0], dst_ref=carried, send_sem=send3, recv_sem=recv3,
        device_id=(after, c), device_id_type=MESH,
    )
    for q in order:
        total = mine[q, 0]
        for o in range(1, chips):
            second[q, o].wait_recv()
            total = total + arrived[q, o - 1]
        if q == 3:
            mine[q, 0] = total
            carry.start()
        elif q > 0:
            out_ref[q] = total
        else:
            carry.wait_recv()
            out_ref[q] = total + carried[...]
    for copy in first.values():
        copy.wait_send()
    for copy in second.values():
        copy.wait_send()
    carry.wait_send()


def exchange(window, n_row, n_col):
    width = window.shape[-1]
    half = width // 2
    rows = half // n_col
    chips = n_col // 2
    dma = pltpu.SemaphoreType.DMA
    return pl.pallas_call(
        functools.partial(exchange_kernel, n_row, n_col),
        out_shape=jax.ShapeDtypeStruct((3, rows, half), jnp.float32),
        in_specs=[pl.BlockSpec(memory_space=pl.ANY)],
        out_specs=pl.BlockSpec(memory_space=pltpu.VMEM),
        scratch_shapes=[
            pltpu.VMEM((4, chips, rows, half), jnp.float32),
            pltpu.VMEM((4, chips, rows, half), jnp.float32),
            pltpu.VMEM((4, chips - 1, rows, half), jnp.float32),
            pltpu.VMEM((rows, half), jnp.float32),
            dma((4, chips)), dma((4, chips)), dma((4, chips)),
            dma((4, chips - 1)), dma((4, chips - 1)),
            dma, dma,
        ],
        compiler_params=pltpu.CompilerParams(
            collective_id=0, has_side_effects=True, vmem_limit_bytes=60 * 2**20
        ),
    )(window.reshape(2, n_col, rows, width))


def on_device(interior_factor, coupling_in, coupling_back, interface_block, gran_count, gran_index):
    n_row, n_col = lax.axis_size("row"), lax.axis_size("col")
    r, c = lax.axis_index("row"), lax.axis_index("col")
    window = None
    for member in range(gran_count.shape[2]):
        count = gran_count[r, c, member]
        index = gran_index[r, c, member]
        slots = jnp.arange(index.shape[0], dtype=jnp.int32)
        slot = jnp.sum(jnp.where(index[:, None] == slots[None, :], slots[:, None], 0), axis=0, dtype=jnp.int32)
        live = (slot < count).astype(jnp.int32)
        part = assemble(
            slot, live, interior_factor[0, 0, member], coupling_in[0, 0, member],
            coupling_back[0, 0, member], interface_block[0, 0, member],
        )
        window = part if window is None else window + part
    return exchange(window, n_row, n_col)[None]


def solution(mesh):
    spec = P("row", "col", None, None, None)
    return jax.shard_map(
        on_device, mesh=mesh, in_specs=(spec, spec, spec, spec, P(), P()),
        out_specs=P("row", None, "col", None), check_vma=False,
    )
```

```python
import functools

import jax
import jax.numpy as jnp
from jax import lax
from jax.experimental import pallas as pl
from jax.experimental.pallas import tpu as pltpu
from jax.sharding import PartitionSpec as P

MESH = pl.DeviceIdType.MESH
HIGHEST = lax.Precision.HIGHEST


def exact_dot(a, b):
    return jnp.dot(a, b, precision=HIGHEST, preferred_element_type=jnp.float32)


def invert_tile(tile):
    size = tile.shape[0]
    i = lax.broadcasted_iota(jnp.int32, tile.shape, 0)
    j = lax.broadcasted_iota(jnp.int32, tile.shape, 1)
    inverse = jnp.where(i == j, 1.0 / jnp.where(i == j, tile, 1.0), 0.0)
    k = 1
    while k < size:
        both = 2 * k
        mask = (i // both == j // both) & (i % both >= k) & (j % both < k)
        below = jnp.where(mask, tile, 0.0)
        inverse = inverse - exact_dot(inverse, exact_dot(below, inverse))
        k = both
    return inverse


def invert_lower(factor_ref, tile, inverse_refs):
    count = factor_ref.shape[0] // tile
    at = lambda b: pl.ds(b * tile, tile)
    diagonal = [invert_tile(factor_ref[at(b), at(b)]) for b in range(count)]
    tiles = {}
    for col in range(count):
        tiles[col, col] = diagonal[col]
        for row in range(col + 1, count):
            total = exact_dot(factor_ref[at(row), at(col)], tiles[col, col])
            for mid in range(col + 1, row):
                total = total + exact_dot(factor_ref[at(row), at(mid)], tiles[mid, col])
            tiles[row, col] = -exact_dot(diagonal[row], total)
    for row in range(count):
        for col in range(count):
            rest = tiles[row, col] if col <= row else jnp.zeros((tile, tile), jnp.float32)
            for ref in inverse_refs:
                piece = rest.astype(jnp.bfloat16)
                ref[at(row), at(col)] = piece
                rest = rest - piece.astype(jnp.float32)


def assemble_kernel(
    granule, tile, slot_ref, live_ref, factor_ref, in_ref, back_ref, own_ref, out_ref,
    high_ref, mid_ref, low_ref, placed_in, placed_back,
):
    wing = placed_in.shape[1] // granule
    p = pl.program_id(0)

    def granule_of(ref, q):
        return ref[:, pl.ds(pl.multiple_of(slot_ref[q] * granule, granule), granule)]

    @pl.when(p == 0)
    def _():
        invert_lower(factor_ref, tile, (high_ref, mid_ref, low_ref))
        step = 4 if wing % 4 == 0 else 1
        for source, target in ((in_ref, placed_in), (back_ref, placed_back)):
            for first in range(0, wing, step):
                pieces = []
                for q in range(first, first + step):
                    piece = granule_of(source, q)
                    pieces.append(jnp.where(live_ref[q] == 1, piece, jnp.zeros_like(piece)))
                coupling = jnp.concatenate(pieces, axis=1) if step > 1 else pieces[0]
                solved = sum(
                    jnp.dot(ref[...], coupling, preferred_element_type=jnp.float32)
                    for ref in (low_ref, mid_ref, high_ref)
                )
                target[:, pl.ds(first * granule, step * granule)] = solved.astype(jnp.bfloat16)

    @pl.when(live_ref[p] == 1)
    def _():
        columns = placed_back[:, pl.ds(pl.multiple_of(p * granule, granule), granule)]
        product = lax.dot_general(
            columns, placed_in[...], (((0,), (0,)), ((), ())), preferred_element_type=jnp.float32
        )
        for q in range(wing):
            block = granule_of(own_ref, q).astype(jnp.float32)
            block = jnp.where(live_ref[q] == 1, block, 0.0)
            out_ref[:, q * granule:(q + 1) * granule] = (
                block - product[:, q * granule:(q + 1) * granule]
            )

    @pl.when(live_ref[p] != 1)
    def _():
        out_ref[...] = jnp.zeros_like(out_ref)


def assemble(slot, live, factor, inner, back, own):
    ni, width = inner.shape
    wing = slot.shape[0]
    granule = width // wing
    tile = 128 if ni % 128 == 0 else ni
    whole = lambda shape: pl.BlockSpec(shape, lambda p, s, l: (0, 0))
    return pl.pallas_call(
        functools.partial(assemble_kernel, granule, tile),
        grid_spec=pltpu.PrefetchScalarGridSpec(
            num_scalar_prefetch=2,
            grid=(wing,),
            in_specs=[
                whole((ni, ni)),
                whole((ni, width)),
                whole((ni, width)),
                pl.BlockSpec((granule, width), lambda p, s, l: (s[p], 0)),
            ],
            out_specs=pl.BlockSpec((granule, width), lambda p, s, l: (p, 0)),
            scratch_shapes=[pltpu.VMEM((ni, ni), jnp.bfloat16)] * 3
            + [pltpu.VMEM((ni, width), jnp.bfloat16)] * 2,
        ),
        out_shape=jax.ShapeDtypeStruct((width, width), jnp.float32),
        compiler_params=pltpu.CompilerParams(vmem_limit_bytes=60 * 2**20),
    )(slot, live, factor, inner, back, own)


LEVELS = 32767.0


def encode(values, group):
    codes, sizes = [], []
    for first in range(0, values.shape[0], group):
        part = values[first:first + group]
        size = jnp.maximum(jnp.max(jnp.abs(part), axis=0, keepdims=True), 1e-33)
        codes.append(jnp.round(part * (LEVELS / size)).astype(jnp.int32).astype(jnp.int16))
        sizes.append(size)
    return codes, sizes


def decode(code_ref, size_ref, at, group):
    parts = []
    for g in range(code_ref.shape[-2] // group):
        code = code_ref[at + (pl.ds(g * group, group),)].astype(jnp.int32).astype(jnp.float32)
        parts.append(code * (size_ref[at + (pl.ds(g, 1),)] * (1.0 / LEVELS)))
    return parts[0] if len(parts) == 1 else jnp.concatenate(parts, axis=0)


def exchange_kernel(
    n_row, n_col, w_ref, out_ref,
    mine, paired, codes, sizes, arrived, arrived_sizes, carried,
    load_sem, send1, recv1, send2, recv2, send_size, recv_size, send3, recv3,
):
    chips = n_col // 2
    rows, half = mine.shape[2], mine.shape[3]
    r = lax.axis_index("row")
    c = lax.axis_index("col")
    chip, core = c // 2, c % 2
    partner = chip * 2 + (1 - core)
    after = lax.rem(r + 1, n_row)
    before = lax.rem(r + n_row - 1, n_row)

    barrier = pltpu.get_barrier_semaphore()
    greet = [(r, partner), (after, c), (before, c)]
    greet += [(r, lax.rem(chip + o, chips) * 2 + core) for o in range(1, chips)]
    for device in greet:
        pl.semaphore_signal(barrier, inc=1, device_id=device, device_id_type=MESH)

    order = [3, 2, 1, 0]
    offsets = list(range(1, chips)) + [0]

    def part(q, o, which):
        device = lax.rem(chip + o, chips) * 2 + which
        return w_ref.at[q // 2, device, :, pl.ds((q % 2) * half, half)]

    group = min(128, rows)
    loads, first, second, second_size = {}, {}, {}, {}
    for q in order:
        for o in offsets:
            loads[q, o] = pltpu.make_async_copy(part(q, o, core), mine.at[q, o], load_sem.at[q, o])
            loads[q, o].start()
    pl.semaphore_wait(barrier, len(greet))
    for q in order:
        for o in offsets:
            first[q, o] = pltpu.make_async_remote_copy(
                src_ref=part(q, o, 1 - core), dst_ref=paired.at[q, o],
                send_sem=send1.at[q, o], recv_sem=recv1.at[q, o],
                device_id=(r, partner), device_id_type=MESH,
            )
            first[q, o].start()
    for q in order:
        for o in offsets:
            loads[q, o].wait()
            first[q, o].wait_recv()
            if not o:
                mine[q, o] = mine[q, o] + paired[q, o]
            else:
                new_codes, new_sizes = encode(mine[q, o] + paired[q, o], group)
                for g in range(len(new_codes)):
                    codes[q, o - 1, pl.ds(g * group, group)] = new_codes[g]
                    sizes[q, o - 1, pl.ds(g, 1)] = new_sizes[g]
                device = lax.rem(chip + o, chips) * 2 + core
                second[q, o] = pltpu.make_async_remote_copy(
                    src_ref=codes.at[q, o - 1], dst_ref=arrived.at[q, o - 1],
                    send_sem=send2.at[q, o - 1], recv_sem=recv2.at[q, o - 1],
                    device_id=(r, device), device_id_type=MESH,
                )
                second[q, o].start()
                second_size[q, o] = pltpu.make_async_remote_copy(
                    src_ref=sizes.at[q, o - 1], dst_ref=arrived_sizes.at[q, o - 1],
                    send_sem=send_size.at[q, o - 1], recv_sem=recv_size.at[q, o - 1],
                    device_id=(r, device), device_id_type=MESH,
                )
                second_size[q, o].start()
    carry = pltpu.make_async_remote_copy(
        src_ref=mine.at[3, 0], dst_ref=carried, send_sem=send3, recv_sem=recv3,
        device_id=(after, c), device_id_type=MESH,
    )
    for q in order:
        total = mine[q, 0]
        for o in range(1, chips):
            second[q, o].wait_recv()
            second_size[q, o].wait_recv()
            total = total + decode(arrived, arrived_sizes, (q, o - 1), group)
        if q == 3:
            mine[q, 0] = total
            carry.start()
        elif q > 0:
            out_ref[q] = total
        else:
            carry.wait_recv()
            out_ref[q] = total + carried[...]
    for copy in first.values():
        copy.wait_send()
    for copy in [*second.values(), *second_size.values()]:
        copy.wait_send()
    carry.wait_send()


def exchange(window, n_row, n_col):
    width = window.shape[-1]
    half = width // 2
    rows = half // n_col
    chips = n_col // 2
    groups = rows // min(128, rows)
    dma = pltpu.SemaphoreType.DMA
    return pl.pallas_call(
        functools.partial(exchange_kernel, n_row, n_col),
        out_shape=jax.ShapeDtypeStruct((3, rows, half), jnp.float32),
        in_specs=[pl.BlockSpec(memory_space=pl.ANY)],
        out_specs=pl.BlockSpec(memory_space=pltpu.VMEM),
        scratch_shapes=[
            pltpu.VMEM((4, chips, rows, half), jnp.float32),
            pltpu.VMEM((4, chips, rows, half), jnp.float32),
            pltpu.VMEM((4, chips - 1, rows, half), jnp.int16),
            pltpu.VMEM((4, chips - 1, groups, half), jnp.float32),
            pltpu.VMEM((4, chips - 1, rows, half), jnp.int16),
            pltpu.VMEM((4, chips - 1, groups, half), jnp.float32),
            pltpu.VMEM((rows, half), jnp.float32),
            dma((4, chips)), dma((4, chips)), dma((4, chips)),
            dma((4, chips - 1)), dma((4, chips - 1)),
            dma((4, chips - 1)), dma((4, chips - 1)),
            dma, dma,
        ],
        compiler_params=pltpu.CompilerParams(
            collective_id=0, has_side_effects=True, vmem_limit_bytes=60 * 2**20
        ),
    )(window.reshape(2, n_col, rows, width))


def on_device(interior_factor, coupling_in, coupling_back, interface_block, gran_count, gran_index):
    n_row, n_col = lax.axis_size("row"), lax.axis_size("col")
    r, c = lax.axis_index("row"), lax.axis_index("col")
    window = None
    for member in range(gran_count.shape[2]):
        count = gran_count[r, c, member]
        index = gran_index[r, c, member]
        slots = jnp.arange(index.shape[0], dtype=jnp.int32)
        slot = jnp.sum(jnp.where(index[:, None] == slots[None, :], slots[:, None], 0), axis=0, dtype=jnp.int32)
        live = (slot < count).astype(jnp.int32)
        part = assemble(
            slot, live, interior_factor[0, 0, member], coupling_in[0, 0, member],
            coupling_back[0, 0, member], interface_block[0, 0, member],
        )
        window = part if window is None else window + part
    return exchange(window, n_row, n_col)[None]


def solution(mesh):
    spec = P("row", "col", None, None, None)
    return jax.shard_map(
        on_device, mesh=mesh, in_specs=(spec, spec, spec, spec, P(), P()),
        out_specs=P("row", None, "col", None), check_vma=False,
    )
```
